128 devices in a mesh: row: 4 (over z), col: 32 (over x, y, core).
Axes of the slice: x: 4, y: 4, z: 4, core: 2. Of those that a mesh axis runs over, the one named last changes fastest.
Arguments:
- neighbor: int32 [32, 3072, 3072], P(None, 'col', 'row'), may hold values from 0 to 1, as said below
- true_coords: float32 [32, 3, 3072], P(None, None, ('row', 'col')), as said below
- pred_coords: float32 [32, 3, 3072], P(None, None, ('row', 'col')), as said below
- residue_mask: int32 [32, 3072], P(None, ('row', 'col')), may hold values from 0 to 1, as said below
- single: bfloat16 [32, 3072, 384], P(None, ('row', 'col'))
- ln_gain: float32 [384], replicated, may hold values from 0.1 to 1.9
- w_hidden: bfloat16 [384, 128], replicated, may hold values from -0.3125 to 0.3125
- b_hidden: float32 [128], replicated, may hold values from -3 to 3
- w_mid: bfloat16 [128, 128], replicated, may hold values from -0.5 to 0.5
- b_mid: float32 [128], replicated, may hold values from -3 to 3
- w_logits: bfloat16 [128, 50], replicated, may hold values from -1.5 to 1.5
- b_logits: float32 [50], replicated, may hold values from -4 to 4
Outputs:
- lddt_score: float32 [32, 3072], P(None, ('row', 'col'))
- residue_loss: float32 [32, 3072], P(None, ('row', 'col'))
- total_loss: float32 [], replicated
The draws below stay inside these ranges and needn't reach their ends.
Inputs may be any that keep to these rules, and one draw needn't show every extreme that they name: `neighbor`: 0 or 1; 0 where j == i; 1 wherever 0 < |i - j| <= 8. `residue_mask`: per structure, 1 on a leading run of 1536 or more residues and 0 after it. `true_coords`: positions in angstroms. `pred_coords`: positions in angstroms.
All inputs are finite; a program needn't handle non-finite values.
Results may differ from the reference program's by a relative error of at most 0.00098.
Values sent between devices are 32-bit elements; how exact they have to be, the bound alone decides.
A program may use at most 64 MiB of HBM per device.

```python
import math
import jax
import jax.numpy as jnp
from jax import lax

L = 3072
BATCH = 32
C_S = 384
HEAD_WIDTH = 128
BINS = 50


def chain_pair(key):
    base = jax.random.fold_in(key, 7)
    k_step, k_scale, k_noise = jax.random.split(base, 3)
    steps = jax.random.normal(k_step, (BATCH, 3, L), jnp.float32) * 2.2
    truth = jnp.cumsum(steps, axis=2)
    scale = jnp.exp(jax.random.uniform(k_scale, (BATCH, 1, L), jnp.float32, math.log(0.3), math.log(6.0)))
    noise = jax.random.normal(k_noise, (BATCH, 3, L), jnp.float32)
    return (truth, truth + scale * noise)


def draw_true_coords(key, part):
    return chain_pair(key)[0]


def draw_pred_coords(key, part):
    return chain_pair(key)[1]


def draw_neighbor(key, part):
    base = jax.random.fold_in(key, 13)
    rows_index = jnp.arange(L)[:, None]
    cols_index = jnp.arange(L)[None, :]
    apart = jnp.abs(rows_index - cols_index)
    banded = (apart <= 8) & (apart > 0)
    chosen = jax.random.randint(base, (BATCH, L, L), 0, 48) == 0
    linked = (banded[None] | chosen) & (apart > 0)[None]
    return jnp.where(linked, 1, 0).astype(jnp.int32)


def draw_residue_mask(key, part):
    base = jax.random.fold_in(key, 17)
    lengths = jax.random.randint(base, (BATCH, 1), L // 2, L + 1)
    positions = jnp.arange(L)[None, :]
    return jnp.where(positions < lengths, 1, 0).astype(jnp.int32)


def draw_single(key, part):
    base = jax.random.fold_in(key, 3)
    k_value = jax.random.fold_in(base, 0)
    values = jax.random.normal(k_value, (BATCH, L, C_S), jnp.float32)
    return values.astype(jnp.bfloat16)


def normal_values(own_key, extent, width, most, dtype=jnp.bfloat16):
    drawn = width * jax.random.normal(own_key, extent, jnp.float32)
    return jnp.clip(drawn, min=-most, max=most).astype(dtype)


def setup_inputs(seed: int = 0) -> dict:
    arg_keys = jax.random.split(jax.random.key(seed), 13)
    return {
        "neighbor": draw_neighbor(jax.random.fold_in(arg_keys[12], 71), 0),
        "true_coords": draw_true_coords(jax.random.fold_in(arg_keys[12], 71), 0),
        "pred_coords": draw_pred_coords(jax.random.fold_in(arg_keys[12], 71), 0),
        "residue_mask": draw_residue_mask(jax.random.fold_in(arg_keys[12], 71), 0),
        "single": draw_single(jax.random.fold_in(arg_keys[12], 71), 0),
        "ln_gain": jnp.clip(1.0 + 0.18 * jax.random.normal(arg_keys[5], (C_S,), jnp.float32), 0.1, 1.9),
        "w_hidden": normal_values(arg_keys[6], (C_S, HEAD_WIDTH), C_S ** -0.5, 0.3125),
        "b_hidden": normal_values(arg_keys[7], (HEAD_WIDTH,), 0.5, 3.0, jnp.float32),
        "w_mid": normal_values(arg_keys[8], (HEAD_WIDTH, HEAD_WIDTH), HEAD_WIDTH ** -0.5, 0.5),
        "b_mid": normal_values(arg_keys[9], (HEAD_WIDTH,), 0.5, 3.0, jnp.float32),
        "w_logits": normal_values(arg_keys[10], (HEAD_WIDTH, BINS), 0.25, 1.5),
        "b_logits": normal_values(arg_keys[11], (BINS,), 1.0, 4.0, jnp.float32),
    }


THRESHOLDS = (0.5, 1.0, 2.0, 4.0)

def pair_dist(near, far):
    total = (near[0][:, None] - far[0][None, :]) ** 2
    total = total + (near[1][:, None] - far[1][None, :]) ** 2
    total = total + (near[2][:, None] - far[2][None, :]) ** 2
    return jnp.sqrt(total + 1e-10)

def soft_preserved(true_dist, pred_dist):
    mismatch = jnp.abs(pred_dist - true_dist)
    scores = jnp.zeros_like(mismatch)
    for threshold in THRESHOLDS:
        scores = scores + jax.nn.sigmoid(4.0 * (threshold - mismatch))
    return 0.25 * scores

def head_loss(lddt_value, single, ln_gain, w_hidden, b_hidden, w_mid, b_mid, w_logits, b_logits):
    features = single.astype(jnp.float32)
    average = lax.optimization_barrier(jnp.mean(features, axis=-1, keepdims=True))
    centred = features - average
    variance = lax.optimization_barrier(jnp.mean(centred * centred, axis=-1, keepdims=True))
    normed = (centred * lax.rsqrt(variance + 1e-05) * ln_gain).astype(jnp.bfloat16)
    first_hidden = jax.nn.relu(jnp.dot(normed, w_hidden, preferred_element_type=jnp.float32) + b_hidden).astype(jnp.bfloat16)
    second_hidden = jax.nn.relu(jnp.dot(first_hidden, w_mid, preferred_element_type=jnp.float32) + b_mid).astype(jnp.bfloat16)
    logits = jnp.dot(second_hidden, w_logits, preferred_element_type=jnp.float32) + b_logits
    log_total = jnp.log(lax.optimization_barrier(jnp.sum(jnp.exp(logits), axis=-1)))
    bins = logits.shape[-1]
    centers = (jnp.arange(bins).astype(jnp.float32) + 0.5) / bins
    closeness = jnp.exp(-(lddt_value[..., None] - centers) ** 2 * (bins * bins * 0.5))
    target = closeness / lax.optimization_barrier(jnp.sum(closeness, axis=-1, keepdims=True))
    return log_total - lax.optimization_barrier(jnp.sum(target * logits, axis=-1))

def reference(neighbor, true_coords, pred_coords, residue_mask, single, ln_gain, w_hidden, b_hidden, w_mid, b_mid, w_logits, b_logits):
    valid = residue_mask.astype(jnp.float32)

    def per_structure(items):
        contacts, truth, guess, keep = items
        scores = soft_preserved(pair_dist(truth, truth), pair_dist(guess, guess))
        weights = contacts.astype(jnp.float32) * keep[None, :] * keep[:, None]
        return (lax.optimization_barrier(jnp.sum(weights * scores, axis=0)), lax.optimization_barrier(jnp.sum(weights, axis=0)))
    preserved, neighbors = lax.map(per_structure, (neighbor, true_coords, pred_coords, valid))
    lddt_score = preserved / jnp.maximum(neighbors, 1.0)
    residue_loss = valid * head_loss(lddt_score, single, ln_gain, w_hidden, b_hidden, w_mid, b_mid, w_logits, b_logits)
    total_loss = jnp.sum(residue_loss) / jnp.sum(valid)
    return (lddt_score, residue_loss, total_loss)
```

```python
import functools

import jax
import jax.numpy as jnp
from jax import lax
from jax.experimental import pallas as pl
from jax.experimental.pallas import tpu as pltpu
from jax.sharding import PartitionSpec as P

B = 32
L = 3072
ROWS = 768
COLS = 96
OWN = 24
HALF = 384
BINS = 50
MESH = pl.DeviceIdType.MESH
SPLIT = 12


def plane(x, y, k):
    return x * 8 + y * 2 + k


def kernel(
    n_hbm, tc_hbm, pc_hbm, mask_hbm, single_hbm, gain_hbm, wh_hbm, bh_hbm, wm_hbm, bm_hbm, wl_hbm, bl_hbm,
    lddt_out, loss_out, total_out,
    nbuf, tc, pc, mask, single, gain, wh, bh, wm, bm, wl, bl,
    blk, rows, zbuf, colbuf, rt, logits, stats, logz, pr, rs_send, rs_recv, ar_send, ar_buf,
    in_sem, n_sem, w_sem, z_ssem, z_rsem, c_ssem, c_rsem, g_ssem, g_rsem, f_ssem, f_rsem,
    rs_ssem, rs_rsem, ar_ssem, ar_rsem,
):
    z = lax.axis_index("row")
    c = lax.axis_index("col")
    x = lax.div(c, 8)
    y = lax.rem(lax.div(c, 2), 4)
    k = lax.rem(c, 2)
    half = lax.div(x, 2)
    other = 1 - half
    partner = plane(x, y, 1 - k)
    lane = lax.broadcasted_iota(jnp.int32, (1, 128), 1)

    barrier = pltpu.get_barrier_semaphore()
    starts = [
        pltpu.make_async_copy(tc_hbm, tc, in_sem.at[0]),
        pltpu.make_async_copy(pc_hbm, pc, in_sem.at[1]),
        pltpu.make_async_copy(mask_hbm, mask, in_sem.at[2]),
    ]
    for s in starts:
        s.start()
    for d in range(1, 4):
        pl.semaphore_signal(barrier, inc=1, device_id=(lax.rem(z + d, 4), c), device_id_type=MESH)
    for d in range(1, 32):
        pl.semaphore_signal(barrier, inc=1, device_id=(z, lax.rem(c + d, 32)), device_id_type=MESH)
    head = [
        pltpu.make_async_copy(a, b, w_sem.at[i])
        for i, (a, b) in enumerate(
            [(single_hbm, single), (gain_hbm, gain), (wh_hbm, wh), (bh_hbm, bh), (wm_hbm, wm), (bm_hbm, bm), (wl_hbm, wl), (bl_hbm, bl)]
        )
    ]
    for s in head:
        s.start()
    n_copies = [pltpu.make_async_copy(n_hbm.at[pl.ds(i * 4, 4)], nbuf.at[pl.ds(i * 4, 4)], n_sem.at[i]) for i in range(8)]
    for s in n_copies:
        s.start()
    for s in starts:
        s.wait()
    valid = mask[...].astype(jnp.float32)
    for i in range(3):
        blk[0, :, i * 32 : (i + 1) * 32] = tc[i] * 2.0
        blk[1, :, i * 32 : (i + 1) * 32] = pc[i] * 2.0
    blk[0, :, 96:128] = valid
    blk[1, :, 96:128] = valid
    own_rows = pl.ds(pl.multiple_of(c * OWN, 8), OWN)
    rows[:, own_rows, :] = blk[...]
    pl.semaphore_wait(barrier, 34)

    def z_copy(d):
        return pltpu.make_async_remote_copy(
            blk, zbuf.at[d], z_ssem.at[d], z_rsem.at[d], device_id=(lax.rem(z + 4 - d, 4), c), device_id_type=MESH
        )

    for d in range(1, 4):
        z_copy(d).start()
    slot = lax.rem(y, 2) * 2 + k
    slot_rows = pl.ds(pl.multiple_of(slot * OWN, 8), OWN)

    def col_send(src, d):
        zz = lax.rem(z + d, 4)
        to = plane(zz, x, lax.div(y, 2))
        copy = pltpu.make_async_remote_copy(
            src, colbuf.at[:, slot_rows, :], c_ssem.at[d], c_rsem.at[slot], device_id=(z, to), device_id_type=MESH
        )
        return to, copy

    def col_start(src, d):
        to, copy = col_send(src, d)

        @pl.when(to != c)
        def _():
            copy.start()

        @pl.when(to == c)
        def _():
            colbuf[:, slot_rows, :] = src[...]

    def row_copy(d):
        xx = jnp.where(d < 8, half, other) * 2 + lax.rem(x + lax.rem(lax.div(d, 4), 2), 2)
        to = plane(xx, lax.rem(y + lax.rem(d, 4), 4), k)
        return pltpu.make_async_remote_copy(
            blk, rows.at[:, own_rows, :], g_ssem.at[d], g_rsem.at[c], device_id=(z, to), device_id_type=MESH
        )

    def row_source(d):
        xx = jnp.where(d < 8, half, other) * 2 + lax.rem(x + lax.rem(lax.div(d, 4), 2), 2)
        return plane(xx, lax.rem(y + lax.rem(d, 4), 4), k)

    def forward(src_c, d):
        at = pl.ds(pl.multiple_of(src_c * OWN, 8), OWN)
        sem = 0 if d < 8 else 1
        return pltpu.make_async_remote_copy(
            rows.at[:, at, :], rows.at[:, at, :], f_ssem.at[sem], f_rsem.at[sem], device_id=(z, partner), device_id_type=MESH
        )

    def row_arrival(src_c, d):
        at = pl.ds(pl.multiple_of(src_c * OWN, 8), OWN)
        pltpu.make_async_remote_copy(
            rows.at[:, at, :], rows.at[:, at, :], g_ssem.at[d], g_rsem.at[src_c], device_id=(z, partner), device_id_type=MESH
        ).wait_recv()

    col_start(blk, 0)
    pltpu.make_async_remote_copy(
        blk, rows.at[:, own_rows, :], f_ssem.at[0], f_rsem.at[0], device_id=(z, partner), device_id_type=MESH
    ).start()
    for d in range(1, 16):
        row_copy(d).start()

    for s in head:
        s.wait()
    feats = single[...].astype(jnp.float32)
    average = jnp.sum(feats, axis=-1, keepdims=True) * (1.0 / 384)
    centred = feats - average
    variance = jnp.sum(centred * centred, axis=-1, keepdims=True) * (1.0 / 384)
    normed = (centred * lax.rsqrt(variance + 1e-05) * gain[...]).astype(jnp.bfloat16)
    first = jnp.maximum(jnp.dot(normed, wh[...], preferred_element_type=jnp.float32) + bh[...], 0.0).astype(jnp.bfloat16)
    second = jnp.maximum(jnp.dot(first, wm[...], preferred_element_type=jnp.float32) + bm[...], 0.0).astype(jnp.bfloat16)
    for g in range(6):
        at = lax.broadcasted_iota(jnp.int32, (1, 128), 1) + g * 128
        source = lax.bitwise_and(at, 31) * OWN + lax.shift_right_logical(at, 5)
        pick = (lax.broadcasted_iota(jnp.int32, (ROWS, 128), 0) == source).astype(jnp.float32).astype(jnp.bfloat16)
        moved = lax.dot_general(second, pick, (((0,), (0,)), ((), ())), preferred_element_type=jnp.float32)
        logits[:, g * 128 : (g + 1) * 128] = jnp.dot(wl[...], moved.astype(jnp.bfloat16), preferred_element_type=jnp.float32)
    eye = lax.broadcasted_iota(jnp.int32, (BINS, BINS), 0) == lax.broadcasted_iota(jnp.int32, (BINS, BINS), 1)
    bias = jnp.sum(jnp.where(eye, bl[...], 0.0), axis=1, keepdims=True)
    with_bias = logits[...] + bias
    logits[...] = with_bias
    top = jnp.max(with_bias, axis=0, keepdims=True)
    logz[...] = top + jnp.log(jnp.sum(jnp.exp(with_bias - top), axis=0, keepdims=True))

    for d in range(1, 4):
        z_copy(d).wait_recv()
        col_start(zbuf.at[d], d)
    for d in range(1, 8):
        src_c = row_source(d)
        row_arrival(src_c, d)
        forward(src_c, d).start()

    def forwards_done(sem):
        pltpu.make_async_remote_copy(
            rows.at[:, pl.ds(0, 8 * OWN), :], rows.at[:, pl.ds(0, 8 * OWN), :], f_ssem.at[sem], f_rsem.at[sem],
            device_id=(z, partner), device_id_type=MESH,
        ).wait_recv()

    forwards_done(0)
    for q in range(4):
        src = plane(y, k * 2 + q // 2, q % 2)
        at = pl.ds(q * OWN, OWN)

        @pl.when(src != c)
        def _():
            pltpu.make_async_remote_copy(
                colbuf.at[:, at, :], colbuf.at[:, at, :], c_ssem.at[0], c_rsem.at[q], device_id=(z, partner), device_id_type=MESH
            ).wait_recv()

    for s in n_copies:
        s.wait()

    def turn(h):
        for t in range(2):
            for g in range(3):
                at = pl.ds(pl.multiple_of(h * HALF + g * 128, 128), 128)
                rt[t * 128 : (t + 1) * 128, g * 128 : (g + 1) * 128] = jnp.transpose(rows[t, at, :])

    def pairs(h):
        lanes = pl.ds(pl.multiple_of(h * HALF, 128), HALF)

        def step(b, _):
            r = [rt[pl.ds(t * 128 + i * 32 + b, 1), :] for t in range(2) for i in range(3)]
            shift = lax.rem(128 - b, 128)
            kept = jnp.zeros((8, HALF), jnp.float32)
            count = jnp.zeros((8, HALF), jnp.float32)
            for g in range(12):
                ct = pltpu.roll(colbuf[0, g * 8 : (g + 1) * 8, :], shift, 1)
                cp = pltpu.roll(colbuf[1, g * 8 : (g + 1) * 8, :], shift, 1)
                w = nbuf[b, g * 8 : (g + 1) * 8, lanes].astype(jnp.float32) * ct[:, 96:97]
                dist = []
                for t, cc in ((0, ct), (1, cp)):
                    dx = cc[:, 0:1] - r[t * 3]
                    dy = cc[:, 32:33] - r[t * 3 + 1]
                    dz = cc[:, 64:65] - r[t * 3 + 2]
                    s = dx * dx + dy * dy + dz * dz + 4e-10
                    dist.append(s * lax.rsqrt(s))
                m = jnp.abs(dist[1] - dist[0])
                v = (jnp.tanh(1.0 - m) + jnp.tanh(2.0 - m)) + (jnp.tanh(4.0 - m) + jnp.tanh(8.0 - m))
                kept = kept + w * v
                count = count + w
            kept1 = jnp.sum(kept, axis=0, keepdims=True)
            count1 = jnp.sum(count, axis=0, keepdims=True)
            pr[pl.ds(b, 1), :] = kept1
            pr[pl.ds(b + 32, 1), :] = count1
            pr[pl.ds(b + 64, 1), :] = kept1
            pr[pl.ds(b + 96, 1), :] = count1
            return 0

        return step

    def rs_copy(h, d):
        to = h * 16 + d
        return to, pltpu.make_async_remote_copy(
            rs_send.at[to], rs_recv.at[c], rs_ssem, rs_rsem, device_id=(z, to), device_id_type=MESH
        )

    def share(h):
        low = lane < 64
        tr = [jnp.transpose(pr[:, g * 128 : (g + 1) * 128]) for g in range(3)]
        unit = lambda u: tr[u // 16][(u % 16) * 8 : (u % 16) * 8 + 8, :]
        for d in range(16):
            rs_send[h * 16 + d, 0:8, :] = jnp.where(low, unit(3 * d), unit(3 * d + 1))
            rs_send[h * 16 + d, 8:16, :] = unit(3 * d + 2)

        def go(d, _):
            to, copy = rs_copy(h, d)

            @pl.when(to != c)
            def _():
                copy.start()

            @pl.when(to == c)
            def _():
                rs_recv[c] = rs_send[c]

            return 0

        lax.fori_loop(0, 16, go, 0)

    turn(half)
    lax.fori_loop(0, SPLIT, pairs(half), 0)
    for d in range(8, 16):
        src_c = row_source(d)
        row_arrival(src_c, d)
        forward(src_c, d).start()
    lax.fori_loop(SPLIT, B, pairs(half), 0)
    share(half)
    forwards_done(1)
    turn(other)
    lax.fori_loop(0, B, pairs(other), 0)
    share(other)

    everyone = lambda a, b: pltpu.make_async_remote_copy(
        rs_send.at[pl.ds(0, 31)], rs_recv.at[pl.ds(0, 31)], rs_ssem, rs_rsem, device_id=(z, partner), device_id_type=MESH
    )
    everyone(0, 0).wait_recv()
    packed = jnp.sum(rs_recv[...], axis=0)
    a0, a1 = packed[0:8], packed[8:16]
    kept = jnp.concatenate([a0, pltpu.roll(a0, 64, 1), a1], axis=0)
    count = pltpu.roll(kept, 96, 1)[:, :32] * valid
    kept = kept[:, :32] * valid
    score = (0.5 * count + 0.125 * kept) / jnp.maximum(count, 1.0)
    lddt_out[...] = score
    stats[0:24, 0:32] = score
    stats[0:24, 32:64] = score
    stats[0:24, 64:96] = score
    stats[0:24, 96:128] = score
    stats[24:48, 0:32] = valid
    stats[24:48, 32:64] = valid
    stats[24:48, 64:96] = valid
    stats[24:48, 96:128] = valid
    group = lax.shift_right_logical(lane, 5)
    centers = (lax.broadcasted_iota(jnp.int32, (BINS, 1), 0).astype(jnp.float32) + 0.5) * (1.0 / BINS)
    loss_sum = jnp.zeros((1, 128), jnp.float32)
    valid_sum = jnp.zeros((1, 128), jnp.float32)
    losses = []
    for g in range(6):
        flat = lambda base: jnp.where(
            group == 0,
            stats[base + 4 * g : base + 4 * g + 1, :],
            jnp.where(
                group == 1,
                stats[base + 4 * g + 1 : base + 4 * g + 2, :],
                jnp.where(group == 2, stats[base + 4 * g + 2 : base + 4 * g + 3, :], stats[base + 4 * g + 3 : base + 4 * g + 4, :]),
            ),
        )
        value, keep = flat(0), flat(24)
        off = value - centers
        near = jnp.exp(off * off * (-(BINS * BINS * 0.5)))
        block = logits[:, g * 128 : (g + 1) * 128]
        mean = jnp.sum(near * block, axis=0, keepdims=True) / jnp.sum(near, axis=0, keepdims=True)
        loss = keep * (logz[:, g * 128 : (g + 1) * 128] - mean)
        losses.append(loss)
        loss_sum = loss_sum + loss
        valid_sum = valid_sum + keep
    both = jnp.where(lane < 64, loss_sum + pltpu.roll(loss_sum, 64, 1), valid_sum + pltpu.roll(valid_sum, 64, 1))
    ar_send[...] = both
    me = z * 32 + c
    ar_buf[pl.ds(me, 1)] = both.reshape(1, 1, 128)
    for d in (2, 1, 3, 0):
        zz = lax.rem(z + d, 4)

        def tell(i, _):
            pltpu.make_async_remote_copy(
                ar_send, ar_buf.at[me], ar_ssem, ar_rsem, device_id=(zz, lax.rem(c + i, 32)), device_id_type=MESH
            ).start()
            return 0

        lax.fori_loop(0 if d else 1, 32, tell, 0)
    for g in range(6):
        for t in range(4):
            part = pltpu.roll(losses[g], (128 - 32 * t) % 128, 1) if t else losses[g]
            loss_out[4 * g + t : 4 * g + t + 1, :] = part[:, :32]

    for d in range(1, 4):
        z_copy(d).wait_send()
    for d in range(4):
        to, copy = col_send(blk, d)

        @pl.when(to != c)
        def _():
            copy.wait_send()

    for d in range(1, 16):
        row_copy(d).wait_send()
    for sem in range(2):
        pltpu.make_async_remote_copy(
            rows.at[:, pl.ds(0, 8 * OWN), :], rows.at[:, pl.ds(0, 8 * OWN), :], f_ssem.at[sem], f_rsem.at[sem],
            device_id=(z, partner), device_id_type=MESH,
        ).wait_send()
    everyone(0, 0).wait_send()
    last = pltpu.make_async_remote_copy(
        ar_buf.at[pl.ds(0, 127)], ar_buf.at[pl.ds(0, 127)], ar_ssem, ar_rsem, device_id=(z, partner), device_id_type=MESH
    )
    last.wait_recv()
    everything = jnp.sum(ar_buf[...], axis=0)
    loss_total = jnp.sum(jnp.where(lane < 64, everything, 0.0), axis=1, keepdims=True)
    valid_total = jnp.sum(jnp.where(lane < 64, 0.0, everything), axis=1, keepdims=True)
    total_out[...] = loss_total / valid_total
    last.wait_send()


def local(neighbor, true_coords, pred_coords, residue_mask, single, ln_gain, w_hidden, b_hidden, w_mid, b_mid, w_logits, b_logits):
    f32, bf16 = jnp.float32, jnp.bfloat16
    anywhere = pl.BlockSpec(memory_space=pl.ANY)
    in_vmem = pl.BlockSpec(memory_space=pltpu.VMEM)
    dma = pltpu.SemaphoreType.DMA
    score, loss, total = pl.pallas_call(
        kernel,
        out_shape=(
            jax.ShapeDtypeStruct((OWN, B), f32),
            jax.ShapeDtypeStruct((OWN, B), f32),
            jax.ShapeDtypeStruct((1, 1), f32),
        ),
        in_specs=[anywhere] * 12,
        out_specs=(in_vmem, in_vmem, in_vmem),
        scratch_shapes=[
            pltpu.VMEM((B, COLS, ROWS), jnp.int32),
            pltpu.VMEM((3, OWN, B), f32),
            pltpu.VMEM((3, OWN, B), f32),
            pltpu.VMEM((OWN, B), jnp.int32),
            pltpu.VMEM((ROWS, 384), bf16),
            pltpu.VMEM((1, 384), f32),
            pltpu.VMEM((384, 128), bf16),
            pltpu.VMEM((1, 128), f32),
            pltpu.VMEM((128, 128), bf16),
            pltpu.VMEM((1, 128), f32),
            pltpu.VMEM((BINS, 128), bf16),
            pltpu.VMEM((1, BINS), f32),
            pltpu.VMEM((2, OWN, 128), f32),
            pltpu.VMEM((2, ROWS, 128), f32),
            pltpu.VMEM((4, 2, OWN, 128), f32),
            pltpu.VMEM((2, COLS, 128), f32),
            pltpu.VMEM((256, HALF), f32),
            pltpu.VMEM((BINS, ROWS), f32),
            pltpu.VMEM((48, 128), f32),
            pltpu.VMEM((1, ROWS), f32),
            pltpu.VMEM((128, HALF), f32),
            pltpu.VMEM((32, 16, 128), f32),
            pltpu.VMEM((32, 16, 128), f32),
            pltpu.VMEM((1, 128), f32),
            pltpu.VMEM((128, 1, 128), f32),
            dma((3,)), dma((8,)), dma((8,)), dma((4,)), dma((4,)), dma((4,)), dma((4,)), dma((16,)), dma((32,)), dma((2,)), dma((2,)),
            dma, dma, dma, dma,
        ],
        compiler_params=pltpu.CompilerParams(collective_id=0, has_side_effects=True, vmem_limit_bytes=48 * 1024 * 1024),
    )(
        neighbor,
        jnp.transpose(true_coords, (1, 2, 0)),
        jnp.transpose(pred_coords, (1, 2, 0)),
        residue_mask.T,
        single.reshape(ROWS, 384),
        ln_gain.reshape(1, 384),
        w_hidden,
        b_hidden.reshape(1, 128),
        w_mid,
        b_mid.reshape(1, 128),
        w_logits.T,
        b_logits.reshape(1, BINS),
    )
    return score.T, loss.T, total.reshape(())


def solution(mesh):
    placed = (
        P(None, "col", "row"),
        P(None, None, ("row", "col")),
        P(None, None, ("row", "col")),
        P(None, ("row", "col")),
        P(None, ("row", "col"), None),
    ) + (P(),) * 7
    return jax.shard_map(
        local,
        mesh=mesh,
        in_specs=placed,
        out_specs=(P(None, ("row", "col")), P(None, ("row", "col")), P()),
        check_vma=False,
    )
```

```python
import functools

import jax
import jax.numpy as jnp
from jax import lax
from jax.experimental import pallas as pl
from jax.experimental.pallas import tpu as pltpu
from jax.sharding import PartitionSpec as P

B = 32
L = 3072
ROWS = 768
COLS = 96
OWN = 24
HALF = 384
BINS = 50
MESH = pl.DeviceIdType.MESH
SPLIT = 3
PITCH = 33


def plane(x, y, k):
    return x * 8 + y * 2 + k


def kernel(
    n_hbm, tc_hbm, pc_hbm, mask_hbm, single_hbm, gain_hbm, wh_hbm, bh_hbm, wm_hbm, bm_hbm, wl_hbm, bl_hbm,
    out,
    nbuf, tc, pc, mask, single, gain, wh, bh, wm, bm, wl, bl,
    blk, rows, zbuf, colbuf, pick_left, left, right, dist, logits, stats, logz, pr, rs_send, rs_recv, ar_send, ar_buf,
    in_sem, n_sem, w_sem, z_ssem, z_rsem, c_ssem, c_rsem, g_ssem, g_rsem, f_ssem, f_rsem,
    rs_ssem, rs_rsem, ar_ssem, ar_rsem, far_in,
):
    z = lax.axis_index("row")
    c = lax.axis_index("col")
    x = lax.div(c, 8)
    y = lax.rem(lax.div(c, 2), 4)
    k = lax.rem(c, 2)
    half = lax.div(x, 2)
    other = 1 - half
    partner = plane(x, y, 1 - k)
    lane = lax.broadcasted_iota(jnp.int32, (1, 128), 1)

    barrier = pltpu.get_barrier_semaphore()
    starts = [
        pltpu.make_async_copy(tc_hbm, tc, in_sem.at[0]),
        pltpu.make_async_copy(pc_hbm, pc, in_sem.at[1]),
        pltpu.make_async_copy(mask_hbm, mask, in_sem.at[2]),
    ]
    for s in starts:
        s.start()
    near = lax.div(x, 2) * 16
    for d in range(1, 4):
        pl.semaphore_signal(barrier, inc=1, device_id=(lax.rem(z + d, 4), c), device_id_type=MESH)
    for d in range(1, 16):
        pl.semaphore_signal(barrier, inc=1, device_id=(z, near + lax.rem(c + d, 16)), device_id_type=MESH)
    mirror = lax.rem(c + 16, 32)
    pl.semaphore_signal(barrier, inc=1, device_id=(z, mirror), device_id_type=MESH)
    head = [
        pltpu.make_async_copy(a, b, w_sem.at[i])
        for i, (a, b) in enumerate(
            [(single_hbm, single), (gain_hbm, gain), (wh_hbm, wh), (bh_hbm, bh), (wm_hbm, wm), (bm_hbm, bm), (wl_hbm, wl), (bl_hbm, bl)]
        )
    ]
    for s in head:
        s.start()
    n_copies = [pltpu.make_async_copy(n_hbm.at[pl.ds(i * 4, 4)], nbuf.at[pl.ds(i * 4, 4)], n_sem.at[i]) for i in range(8)]
    for s in n_copies:
        s.start()
    for s in starts:
        s.wait()
    valid = mask[...].astype(jnp.float32)
    for i in range(3):
        blk[0, :, i * 32 : (i + 1) * 32] = tc[i] * 2.0
        blk[1, :, i * 32 : (i + 1) * 32] = pc[i] * 2.0
    blk[0, :, 96:128] = valid
    blk[1, :, 96:128] = valid
    own_rows = pl.ds(pl.multiple_of(c * OWN, 8), OWN)
    rows[:, own_rows, :] = blk[...]
    pl.semaphore_wait(barrier, 19)
    pl.semaphore_signal(far_in, inc=1, device_id=(z, mirror), device_id_type=MESH)

    def z_copy(d):
        return pltpu.make_async_remote_copy(
            blk, zbuf.at[d], z_ssem.at[d], z_rsem.at[d], device_id=(lax.rem(z + 4 - d, 4), c), device_id_type=MESH
        )

    for d in range(1, 4):
        z_copy(d).start()
    slot = lax.rem(y, 2) * 2 + k
    slot_rows = pl.ds(pl.multiple_of(slot * OWN, 8), OWN)

    def col_send(src, d):
        zz = lax.rem(z + d, 4)
        to = plane(zz, x, lax.div(y, 2))
        copy = pltpu.make_async_remote_copy(
            src, colbuf.at[:, slot_rows, :], c_ssem.at[d], c_rsem.at[slot], device_id=(z, to), device_id_type=MESH
        )
        return to, copy

    def col_start(src, d):
        to, copy = col_send(src, d)

        @pl.when(to != c)
        def _():
            copy.start()

        @pl.when(to == c)
        def _():
            colbuf[:, slot_rows, :] = src[...]

    def row_copy(d):
        xx = jnp.where(d < 8, half, other) * 2 + lax.rem(x + lax.rem(lax.div(d, 4), 2), 2)
        to = plane(xx, lax.rem(y + lax.rem(d, 4), 4), k)
        return pltpu.make_async_remote_copy(
            blk, rows.at[:, own_rows, :], g_ssem.at[d], g_rsem.at[c], device_id=(z, to), device_id_type=MESH
        )

    def row_source(d):
        xx = jnp.where(d < 8, half, other) * 2 + lax.rem(x + lax.rem(lax.div(d, 4), 2), 2)
        return plane(xx, lax.rem(y + lax.rem(d, 4), 4), k)

    def forward(src_c, d):
        at = pl.ds(pl.multiple_of(src_c * OWN, 8), OWN)
        sem = 0 if d < 8 else 1
        return pltpu.make_async_remote_copy(
            rows.at[:, at, :], rows.at[:, at, :], f_ssem.at[sem], f_rsem.at[sem], device_id=(z, partner), device_id_type=MESH
        )

    def row_arrival(src_c, d):
        at = pl.ds(pl.multiple_of(src_c * OWN, 8), OWN)
        pltpu.make_async_remote_copy(
            rows.at[:, at, :], rows.at[:, at, :], g_ssem.at[d], g_rsem.at[src_c], device_id=(z, partner), device_id_type=MESH
        ).wait_recv()

    pltpu.make_async_remote_copy(
        blk, rows.at[:, own_rows, :], f_ssem.at[0], f_rsem.at[0], device_id=(z, partner), device_id_type=MESH
    ).start()
    for d in range(1, 8):
        row_copy(d).start()

    pl.semaphore_wait(far_in, 1)
    col_start(blk, 0)
    for d in range(8, 16):
        row_copy(d).start()
    for s in head:
        s.wait()
    feats = single[...].astype(jnp.float32)
    average = jnp.sum(feats, axis=-1, keepdims=True) * (1.0 / 384)
    centred = feats - average
    variance = jnp.sum(centred * centred, axis=-1, keepdims=True) * (1.0 / 384)
    normed = (centred * lax.rsqrt(variance + 1e-05) * gain[...].reshape(1, 384)).astype(jnp.bfloat16)
    first = jnp.maximum(jnp.dot(normed, wh[...], preferred_element_type=jnp.float32) + bh[...], 0.0).astype(jnp.bfloat16)
    second = jnp.maximum(jnp.dot(first, wm[...], preferred_element_type=jnp.float32) + bm[...], 0.0).astype(jnp.bfloat16)
    for g in range(6):
        at = lax.broadcasted_iota(jnp.int32, (1, 128), 1) + g * 128
        source = lax.bitwise_and(at, 31) * OWN + lax.shift_right_logical(at, 5)
        pick = (lax.broadcasted_iota(jnp.int32, (ROWS, 128), 0) == source).astype(jnp.float32).astype(jnp.bfloat16)
        moved = lax.dot_general(second, pick, (((0,), (0,)), ((), ())), preferred_element_type=jnp.float32)
        logits[:, g * 128 : (g + 1) * 128] = jnp.dot(wl[...], moved.astype(jnp.bfloat16), preferred_element_type=jnp.float32)
    eye = lax.broadcasted_iota(jnp.int32, (BINS, BINS), 0) == lax.broadcasted_iota(jnp.int32, (BINS, BINS), 1)
    bias = jnp.sum(jnp.where(eye, bl[...], 0.0), axis=1, keepdims=True)
    with_bias = logits[...] + bias
    logits[...] = with_bias
    top = jnp.max(with_bias, axis=0, keepdims=True)
    logz[...] = top + jnp.log(jnp.sum(jnp.exp(with_bias - top), axis=0, keepdims=True))

    for i in range(16):
        at = lax.broadcasted_iota(jnp.int32, (1, 128), 1) + i * 128
        b_of = lax.shift_right_logical(at, 6)
        q = lax.bitwise_and(lax.shift_right_logical(at, 4), 3)
        p = lax.bitwise_and(lax.shift_right_logical(at, 2), 3)
        part = lax.bitwise_and(at, 3)
        source = jnp.where(
            (p < 3) & (q < 3) & ((part < 3) | (q == 0)),
            p * 128 + part * 32 + b_of,
            jnp.where((part == 3) & (((q == 1) & (p < 2)) | ((q == 2) & (p == 0))), 384, -1),
        )
        hot = (lax.broadcasted_iota(jnp.int32, (512, 128), 0) == source).astype(jnp.float32)
        pick_left[:, i * 128 : (i + 1) * 128] = hot.astype(jnp.bfloat16)

    for d in range(1, 4):
        z_copy(d).wait_recv()
        col_start(zbuf.at[d], d)
    for d in range(1, 8):
        src_c = row_source(d)
        row_arrival(src_c, d)
        forward(src_c, d).start()

    def forwards_done(sem):
        pltpu.make_async_remote_copy(
            rows.at[:, pl.ds(0, 8 * OWN), :], rows.at[:, pl.ds(0, 8 * OWN), :], f_ssem.at[sem], f_rsem.at[sem],
            device_id=(z, partner), device_id_type=MESH,
        ).wait_recv()

    forwards_done(0)
    for q in range(4):
        src = plane(y, k * 2 + q // 2, q % 2)
        at = pl.ds(q * OWN, OWN)

        @pl.when(src != c)
        def _():
            pltpu.make_async_remote_copy(
                colbuf.at[:, at, :], colbuf.at[:, at, :], c_ssem.at[0], c_rsem.at[q], device_id=(z, partner), device_id_type=MESH
            ).wait_recv()

    for s in n_copies:
        s.wait()

    def pieces(v):
        p0 = v.astype(jnp.bfloat16).astype(jnp.float32)
        p1 = (v - p0).astype(jnp.bfloat16).astype(jnp.float32)
        return p0, p1, v - p0 - p1

    def centre(t):
        return jnp.where(lane < 96, colbuf[t, 0:1, :], 0.0)

    def left_sides():
        both = []
        for t in range(2):
            a = colbuf[t] - centre(t)
            sq = a * a
            norm = (pltpu.roll(sq, 96, 1) + pltpu.roll(sq, 64, 1)) + pltpu.roll(sq, 32, 1)
            parts = pieces(jnp.where(lane < 96, a, norm))
            both.append(jnp.concatenate([p.astype(jnp.bfloat16) for p in parts] + [jnp.ones((COLS, 128), jnp.bfloat16)], axis=1))
        both = jnp.concatenate(both, axis=0)
        for i in range(8):
            at = slice(i * 256, (i + 1) * 256)
            left[:, at] = jnp.dot(both, pick_left[:, at], preferred_element_type=jnp.float32).astype(jnp.bfloat16)

    def turn(h):
        one = jnp.full((32, 128), 1.0, jnp.float32)
        for t in range(2):
            mid = centre(t)
            for v in range(3):
                at = pl.ds(pl.multiple_of(h * HALF + v * 128, 128), 128)
                flat = jnp.transpose(rows[t, at, :] - mid)
                xyz = flat[0:96]
                sq = xyz * xyz
                m = pieces((sq[0:32] + sq[32:64]) + (sq[64:96] + 4e-10))
                p = pieces(xyz * -2.0)
                for q, (u, w) in enumerate(((one, one), (m[0], m[1]), (m[2], m[2]))):
                    for slot, rows32 in enumerate((p[q][0:32], p[q][32:64], p[q][64:96], u) + (p[q][0:32], p[q][32:64], p[q][64:96], w)):
                        right[t, q, v, slot * PITCH : slot * PITCH + 32, :] = rows32

    def distances(b, i, s, dst):
        at = pl.ds(pl.multiple_of(i * 128, 128), 128)
        for t in range(2):
            lhs = left[t * COLS : (t + 1) * COLS, at]
            cols = []
            for v in range(3):
                vs = [right[t, q, v, pl.ds(b, 8, stride=PITCH), :] for q in range(3)]
                cols.append(jnp.concatenate([vs[0], vs[0], vs[1], vs[1], vs[2], vs[2]], axis=0).astype(jnp.bfloat16))
            rhs = jnp.concatenate(cols, axis=1)
            if s == 0:
                rhs = jnp.concatenate([rhs, jnp.zeros((80, HALF), jnp.bfloat16)], axis=0)
            else:
                rhs = jnp.concatenate([jnp.zeros((64, HALF), jnp.bfloat16), rhs, jnp.zeros((16, HALF), jnp.bfloat16)], axis=0)
            dst[t] = jnp.dot(lhs, rhs, preferred_element_type=jnp.float32)

    def pairs(h):
        def one(b, src):
            kept = [jnp.zeros((8, 128), jnp.float32)] * 3
            count = [jnp.zeros((8, 128), jnp.float32)] * 3
            shift = lax.rem(128 - b, 128)
            for g in range(12):
                cm = jnp.broadcast_to(pltpu.roll(colbuf[0, g * 8 : (g + 1) * 8, :], shift, 1)[:, 96:97], (8, 128))
                for v in range(3):
                    lanes = pl.ds(pl.multiple_of(h * HALF + v * 128, 128), 128)
                    w = nbuf[b, g * 8 : (g + 1) * 8, lanes].astype(jnp.float32) * cm
                    s0 = jnp.maximum(src[0, g * 8 : (g + 1) * 8, v * 128 : (v + 1) * 128], 4e-10)
                    s1 = jnp.maximum(src[1, g * 8 : (g + 1) * 8, v * 128 : (v + 1) * 128], 4e-10)
                    m = jnp.abs(s1 * lax.rsqrt(s1) - s0 * lax.rsqrt(s0))
                    score = (jnp.tanh(1.0 - m) + jnp.tanh(2.0 - m)) + (jnp.tanh(4.0 - m) + jnp.tanh(8.0 - m))
                    kept[v] = kept[v] + w * score
                    count[v] = count[v] + w
            for v in range(3):
                kept1 = jnp.sum(kept[v], axis=0, keepdims=True)
                count1 = jnp.sum(count[v], axis=0, keepdims=True)
                pr[v, pl.ds(b, 1), :] = kept1
                pr[v, pl.ds(b + 32, 1), :] = count1
                pr[v, pl.ds(b + 64, 1), :] = kept1
                pr[v, pl.ds(b + 96, 1), :] = count1

        def step(i, _):
            after = jnp.minimum(i + 1, B // 4 - 1)

            def quad(now, later):
                for j in range(4):
                    one(4 * i + j, dist.at[now + j])
                for j in range(4):
                    distances(4 * after + j, 2 * after + j // 2, j % 2, dist.at[later + j])

            @pl.when(lax.rem(i, 2) == 0)
            def _():
                quad(0, 4)

            @pl.when(lax.rem(i, 2) == 1)
            def _():
                quad(4, 0)

            return 0

        return step

    def rs_copy(h, d):
        to = h * 16 + d
        return to, pltpu.make_async_remote_copy(
            rs_send.at[to], rs_recv.at[c], rs_ssem, rs_rsem, device_id=(z, to), device_id_type=MESH
        )

    def share(h):
        low = lane < 64
        tr = [jnp.transpose(pr[g]) for g in range(3)]
        unit = lambda u: tr[u // 16][(u % 16) * 8 : (u % 16) * 8 + 8, :]
        for d in range(16):
            rs_send[h * 16 + d, 0:8, :] = jnp.where(low, unit(3 * d), unit(3 * d + 1))
            rs_send[h * 16 + d, 8:16, :] = unit(3 * d + 2)

        for d in range(16):
            to, copy = rs_copy(h, d)

            @pl.when(to != c)
            def _():
                copy.start()

            @pl.when(to == c)
            def _():
                rs_recv[c] = rs_send[c]


    left_sides()
    turn(half)
    for j in range(4):
        distances(j, j // 2, j % 2, dist.at[j])
    lax.fori_loop(0, SPLIT, pairs(half), 0)
    for d in range(8, 16):
        src_c = row_source(d)
        row_arrival(src_c, d)
        forward(src_c, d).start()
    lax.fori_loop(SPLIT, B // 4, pairs(half), 0)
    share(half)
    forwards_done(1)
    turn(other)
    for j in range(4):
        distances(j, j // 2, j % 2, dist.at[j])
    lax.fori_loop(0, B // 4, pairs(other), 0)
    share(other)

    everyone = lambda a, b: pltpu.make_async_remote_copy(
        rs_send.at[pl.ds(0, 31)], rs_recv.at[pl.ds(0, 31)], rs_ssem, rs_rsem, device_id=(z, partner), device_id_type=MESH
    )
    everyone(0, 0).wait_recv()
    packed = jnp.sum(rs_recv[...], axis=0)
    a0, a1 = packed[0:8], packed[8:16]
    kept = jnp.concatenate([a0, pltpu.roll(a0, 64, 1), a1], axis=0)
    count = pltpu.roll(kept, 96, 1)[:, :32] * valid
    kept = kept[:, :32] * valid
    score = (0.5 * count + 0.125 * kept) / jnp.maximum(count, 1.0)
    out[0] = score
    stats[0:24, 0:32] = score
    stats[0:24, 32:64] = score
    stats[0:24, 64:96] = score
    stats[0:24, 96:128] = score
    stats[24:48, 0:32] = valid
    stats[24:48, 32:64] = valid
    stats[24:48, 64:96] = valid
    stats[24:48, 96:128] = valid
    group = lax.shift_right_logical(lane, 5)
    centers = (lax.broadcasted_iota(jnp.int32, (BINS, 1), 0).astype(jnp.float32) + 0.5) * (1.0 / BINS)
    loss_sum = jnp.zeros((1, 128), jnp.float32)
    valid_sum = jnp.zeros((1, 128), jnp.float32)
    losses = []
    for g in range(6):
        flat = lambda base: jnp.where(
            group == 0,
            stats[base + 4 * g : base + 4 * g + 1, :],
            jnp.where(
                group == 1,
                stats[base + 4 * g + 1 : base + 4 * g + 2, :],
                jnp.where(group == 2, stats[base + 4 * g + 2 : base + 4 * g + 3, :], stats[base + 4 * g + 3 : base + 4 * g + 4, :]),
            ),
        )
        value, keep = flat(0), flat(24)
        off = value - centers
        near = jnp.exp(off * off * (-(BINS * BINS * 0.5)))
        block = logits[:, g * 128 : (g + 1) * 128]
        mean = jnp.sum(near * block, axis=0, keepdims=True) / jnp.sum(near, axis=0, keepdims=True)
        loss = keep * (logz[:, g * 128 : (g + 1) * 128] - mean)
        losses.append(loss)
        loss_sum = loss_sum + loss
        valid_sum = valid_sum + keep
    both = jnp.where(lane < 64, loss_sum + pltpu.roll(loss_sum, 64, 1), valid_sum + pltpu.roll(valid_sum, 64, 1))
    ar_send[...] = both
    me = z * 32 + c
    ar_buf[pl.ds(me, 1)] = both.reshape(1, 1, 128)
    for i in range(128):

        @pl.when(me != i)
        def _():
            pltpu.make_async_remote_copy(
                ar_send, ar_buf.at[me], ar_ssem, ar_rsem, device_id=(i // 32, i % 32), device_id_type=MESH
            ).start()

    for g in range(6):
        for t in range(4):
            part = pltpu.roll(losses[g], (128 - 32 * t) % 128, 1) if t else losses[g]
            out[1, 4 * g + t : 4 * g + t + 1, :] = part[:, :32]

    for d in range(1, 4):
        z_copy(d).wait_send()
    for d in range(4):
        to, copy = col_send(blk, d)

        @pl.when(to != c)
        def _():
            copy.wait_send()

    for d in range(1, 16):
        row_copy(d).wait_send()
    for sem in range(2):
        pltpu.make_async_remote_copy(
            rows.at[:, pl.ds(0, 8 * OWN), :], rows.at[:, pl.ds(0, 8 * OWN), :], f_ssem.at[sem], f_rsem.at[sem],
            device_id=(z, partner), device_id_type=MESH,
        ).wait_send()
    everyone(0, 0).wait_send()
    last = pltpu.make_async_remote_copy(
        ar_buf.at[pl.ds(0, 127)], ar_buf.at[pl.ds(0, 127)], ar_ssem, ar_rsem, device_id=(z, partner), device_id_type=MESH
    )
    last.wait_recv()
    everything = jnp.sum(ar_buf[...], axis=0)
    loss_total = jnp.sum(jnp.where(lane < 64, everything, 0.0), axis=1, keepdims=True)
    valid_total = jnp.sum(jnp.where(lane < 64, 0.0, everything), axis=1, keepdims=True)
    out[2] = jnp.broadcast_to(loss_total / valid_total, (OWN, B))
    last.wait_send()


def finish(out, score, loss, total):
    score[...] = out[0]
    loss[...] = out[1]
    total[...] = out[2, 0:1, 0:1]


def local(neighbor, true_coords, pred_coords, residue_mask, single, ln_gain, w_hidden, b_hidden, w_mid, b_mid, w_logits, b_logits):
    f32, bf16 = jnp.float32, jnp.bfloat16
    anywhere = pl.BlockSpec(memory_space=pl.ANY)
    in_vmem = pl.BlockSpec(memory_space=pltpu.VMEM)
    dma = pltpu.SemaphoreType.DMA
    out = pl.pallas_call(
        kernel,
        out_shape=jax.ShapeDtypeStruct((3, OWN, B), f32),
        in_specs=[anywhere] * 12,
        out_specs=in_vmem,
        scratch_shapes=[
            pltpu.VMEM((B, COLS, ROWS), jnp.int32),
            pltpu.VMEM((3, OWN, B), f32),
            pltpu.VMEM((3, OWN, B), f32),
            pltpu.VMEM((OWN, B), jnp.int32),
            pltpu.VMEM((ROWS, 384), bf16),
            pltpu.VMEM((384,), f32),
            pltpu.VMEM((384, 128), bf16),
            pltpu.VMEM((1, 128), f32),
            pltpu.VMEM((128, 128), bf16),
            pltpu.VMEM((1, 128), f32),
            pltpu.VMEM((BINS, 128), bf16),
            pltpu.VMEM((1, BINS), f32),
            pltpu.VMEM((2, OWN, 128), f32),
            pltpu.VMEM((2, ROWS, 128), f32),
            pltpu.VMEM((4, 2, OWN, 128), f32),
            pltpu.VMEM((2, COLS, 128), f32),
            pltpu.VMEM((512, 2048), bf16),
            pltpu.VMEM((2 * COLS, 2048), bf16),
            pltpu.VMEM((2, 3, 3, 8 * PITCH, 128), f32),
            pltpu.VMEM((8, 2, COLS, HALF), f32),
            pltpu.VMEM((BINS, ROWS), f32),
            pltpu.VMEM((48, 128), f32),
            pltpu.VMEM((1, ROWS), f32),
            pltpu.VMEM((3, 128, 128), f32),
            pltpu.VMEM((32, 16, 128), f32),
            pltpu.VMEM((32, 16, 128), f32),
            pltpu.VMEM((1, 128), f32),
            pltpu.VMEM((128, 1, 128), f32),
            dma((3,)), dma((8,)), dma((8,)), dma((4,)), dma((4,)), dma((4,)), dma((4,)), dma((16,)), dma((32,)), dma((2,)), dma((2,)),
            dma, dma, dma, dma, pltpu.SemaphoreType.REGULAR,
        ],
        compiler_params=pltpu.CompilerParams(collective_id=0, has_side_effects=True, vmem_limit_bytes=67043328),
    )(
        neighbor,
        jnp.transpose(true_coords, (1, 2, 0)),
        jnp.transpose(pred_coords, (1, 2, 0)),
        residue_mask.T,
        single.reshape(ROWS, 384),
        ln_gain,
        w_hidden,
        b_hidden.reshape(1, 128),
        w_mid,
        b_mid.reshape(1, 128),
        w_logits.T,
        b_logits.reshape(1, BINS),
    )
    score, loss, total = pl.pallas_call(
        finish,
        out_shape=(jax.ShapeDtypeStruct((OWN, B), f32), jax.ShapeDtypeStruct((OWN, B), f32), jax.ShapeDtypeStruct((1, 1), f32)),
        in_specs=[in_vmem],
        out_specs=(in_vmem, in_vmem, in_vmem),
    )(out)
    return score.T, loss.T, total.reshape(())


def solution(mesh):
    placed = (
        P(None, "col", "row"),
        P(None, None, ("row", "col")),
        P(None, None, ("row", "col")),
        P(None, ("row", "col")),
        P(None, ("row", "col"), None),
    ) + (P(),) * 7
    return jax.shard_map(
        local,
        mesh=mesh,
        in_specs=placed,
        out_specs=(P(None, ("row", "col")), P(None, ("row", "col")), P()),
        check_vma=False,
    )
```

```python
import functools

import jax
import jax.numpy as jnp
from jax import lax
from jax.experimental import pallas as pl
from jax.experimental.pallas import tpu as pltpu
from jax.sharding import PartitionSpec as P

B = 32
L = 3072
ROWS = 768
COLS = 96
OWN = 24
HALF = 384
BINS = 50
MESH = pl.DeviceIdType.MESH
SPLIT = 5
PITCH = 33


def plane(x, y, k):
    return x * 8 + y * 2 + k


def kernel(
    n_hbm, tc_hbm, pc_hbm, mask_hbm, single_hbm, gain_hbm, wh_hbm, bh_hbm, wm_hbm, bm_hbm, wl_hbm, bl_hbm,
    out,
    nbuf, tc, pc, mask, single, gain, wh, bh, wm, bm, wl, bl,
    blk, rblk, rows, zbuf, colbuf, pick_left, left, right, dist, logits, stats, logz, pr, rs_send, rs_recv, ar_send, ar_buf,
    in_sem, n_sem, w_sem, z_ssem, z_rsem, c_ssem, c_rsem, g_ssem, g_rsem, f_ssem, f_rsem,
    rs_ssem, rs_rsem, ar_ssem, ar_rsem, far_in,
):
    z = lax.axis_index("row")
    c = lax.axis_index("col")
    x = lax.div(c, 8)
    y = lax.rem(lax.div(c, 2), 4)
    k = lax.rem(c, 2)
    half = lax.div(x, 2)
    other = 1 - half
    partner = plane(x, y, 1 - k)
    lane = lax.broadcasted_iota(jnp.int32, (1, 128), 1)

    barrier = pltpu.get_barrier_semaphore()
    starts = [
        pltpu.make_async_copy(tc_hbm, tc, in_sem.at[0]),
        pltpu.make_async_copy(pc_hbm, pc, in_sem.at[1]),
        pltpu.make_async_copy(mask_hbm, mask, in_sem.at[2]),
    ]
    for s in starts:
        s.start()
    near = lax.div(x, 2) * 16
    for d in range(1, 4):
        pl.semaphore_signal(barrier, inc=1, device_id=(lax.rem(z + d, 4), c), device_id_type=MESH)
    for d in range(1, 16):
        pl.semaphore_signal(barrier, inc=1, device_id=(z, near + lax.rem(c + d, 16)), device_id_type=MESH)
    mirror = lax.rem(c + 16, 32)
    pl.semaphore_signal(barrier, inc=1, device_id=(z, mirror), device_id_type=MESH)
    head = [
        pltpu.make_async_copy(a, b, w_sem.at[i])
        for i, (a, b) in enumerate(
            [(single_hbm, single), (gain_hbm, gain), (wh_hbm, wh), (bh_hbm, bh), (wm_hbm, wm), (bm_hbm, bm), (wl_hbm, wl), (bl_hbm, bl)]
        )
    ]
    for s in head:
        s.start()
    n_copies = [pltpu.make_async_copy(n_hbm.at[pl.ds(i * 4, 4)], nbuf.at[pl.ds(i * 4, 4)], n_sem.at[i]) for i in range(8)]
    for s in n_copies:
        s.start()
    for s in starts:
        s.wait()
    valid = mask[...].astype(jnp.float32)
    for i in range(3):
        blk[0, :, i * 32 : (i + 1) * 32] = tc[i] * 2.0
        blk[1, :, i * 32 : (i + 1) * 32] = pc[i] * 2.0
    blk[0, :, 96:128] = valid
    blk[1, :, 96:128] = valid
    for i, part in enumerate((tc[0], tc[1], tc[2], pc[0])):
        rblk[0:24, i * 32 : (i + 1) * 32] = part * 2.0
    for i in range(3):
        at = slice(24 + 8 * (i // 2), 32 + 8 * (i // 2))
        for j in range(2):
            lo = (i % 2) * 64 + j * 32
            rblk[at, lo : lo + 32] = pc[1 + j, 8 * i : 8 * i + 8, :] * 2.0
    rblk[32:40, 64:128] = jnp.zeros((8, 64), jnp.float32)
    rows[c] = rblk[...]
    pl.semaphore_wait(barrier, 19)
    pl.semaphore_signal(far_in, inc=1, device_id=(z, mirror), device_id_type=MESH)

    def z_copy(d):
        return pltpu.make_async_remote_copy(
            blk, zbuf.at[d], z_ssem.at[d], z_rsem.at[d], device_id=(lax.rem(z + 4 - d, 4), c), device_id_type=MESH
        )

    for d in range(1, 4):
        z_copy(d).start()
    slot = lax.rem(y, 2) * 2 + k
    slot_rows = pl.ds(pl.multiple_of(slot * OWN, 8), OWN)

    def col_send(src, d):
        zz = lax.rem(z + d, 4)
        to = plane(zz, x, lax.div(y, 2))
        copy = pltpu.make_async_remote_copy(
            src, colbuf.at[:, slot_rows, :], c_ssem.at[d], c_rsem.at[slot], device_id=(z, to), device_id_type=MESH
        )
        return to, copy

    def col_start(src, d):
        to, copy = col_send(src, d)

        @pl.when(to != c)
        def _():
            copy.start()

        @pl.when(to == c)
        def _():
            colbuf[:, slot_rows, :] = src[...]

    def row_copy(d):
        xx = jnp.where(d < 8, half, other) * 2 + lax.rem(x + lax.rem(lax.div(d, 4), 2), 2)
        to = plane(xx, lax.rem(y + lax.rem(d, 4), 4), k)
        return pltpu.make_async_remote_copy(
            rblk, rows.at[c], g_ssem.at[d], g_rsem.at[c], device_id=(z, to), device_id_type=MESH
        )

    def row_source(d):
        xx = jnp.where(d < 8, half, other) * 2 + lax.rem(x + lax.rem(lax.div(d, 4), 2), 2)
        return plane(xx, lax.rem(y + lax.rem(d, 4), 4), k)

    def forward(src_c, d):
        sem = 0 if d < 8 else 1
        return pltpu.make_async_remote_copy(
            rows.at[src_c], rows.at[src_c], f_ssem.at[sem], f_rsem.at[sem], device_id=(z, partner), device_id_type=MESH
        )

    def row_arrival(src_c, d):
        pltpu.make_async_remote_copy(
            rows.at[src_c], rows.at[src_c], g_ssem.at[d], g_rsem.at[src_c], device_id=(z, partner), device_id_type=MESH
        ).wait_recv()

    pltpu.make_async_remote_copy(
        rblk, rows.at[c], f_ssem.at[0], f_rsem.at[0], device_id=(z, partner), device_id_type=MESH
    ).start()
    for d in range(1, 8):
        row_copy(d).start()

    pl.semaphore_wait(far_in, 1)
    col_start(blk, 0)
    for d in range(8, 16):
        row_copy(d).start()
    for i in range(16):
        at = lax.broadcasted_iota(jnp.int32, (1, 128), 1) + i * 128
        b_of = lax.shift_right_logical(at, 6)
        q = lax.bitwise_and(lax.shift_right_logical(at, 4), 3)
        p = lax.bitwise_and(lax.shift_right_logical(at, 2), 3)
        part = lax.bitwise_and(at, 3)
        source = jnp.where(
            (p < 3) & (q < 3) & ((part < 3) | (q == 0)),
            p * 128 + part * 32 + b_of,
            jnp.where((part == 3) & (((q == 1) & (p < 2)) | ((q == 2) & (p == 0))), 384, -1),
        )
        hot = (lax.broadcasted_iota(jnp.int32, (512, 128), 0) == source).astype(jnp.float32)
        pick_left[:, i * 128 : (i + 1) * 128] = hot.astype(jnp.bfloat16)

    for d in range(1, 4):
        z_copy(d).wait_recv()
        col_start(zbuf.at[d], d)
    for d in range(1, 8):
        src_c = row_source(d)
        row_arrival(src_c, d)
        forward(src_c, d).start()

    def forwards_done(sem):
        pltpu.make_async_remote_copy(
            rows.at[pl.ds(0, 8)], rows.at[pl.ds(0, 8)], f_ssem.at[sem], f_rsem.at[sem],
            device_id=(z, partner), device_id_type=MESH,
        ).wait_recv()

    forwards_done(0)
    for q in range(4):
        src = plane(y, k * 2 + q // 2, q % 2)
        at = pl.ds(q * OWN, OWN)

        @pl.when(src != c)
        def _():
            pltpu.make_async_remote_copy(
                colbuf.at[:, at, :], colbuf.at[:, at, :], c_ssem.at[0], c_rsem.at[q], device_id=(z, partner), device_id_type=MESH
            ).wait_recv()

    for s in n_copies:
        s.wait()

    def pieces(v):
        p0 = v.astype(jnp.bfloat16).astype(jnp.float32)
        p1 = (v - p0).astype(jnp.bfloat16).astype(jnp.float32)
        return p0, p1, v - p0 - p1

    def centre(t):
        return jnp.where(lane < 96, colbuf[t, 0:1, :], 0.0)

    def left_sides():
        both = []
        for t in range(2):
            a = colbuf[t] - centre(t)
            sq = a * a
            norm = (pltpu.roll(sq, 96, 1) + pltpu.roll(sq, 64, 1)) + pltpu.roll(sq, 32, 1)
            parts = pieces(jnp.where(lane < 96, a, norm))
            both.append(jnp.concatenate([p.astype(jnp.bfloat16) for p in parts] + [jnp.ones((COLS, 128), jnp.bfloat16)], axis=1))
        both = jnp.concatenate(both, axis=0)
        for i in range(8):
            at = slice(i * 256, (i + 1) * 256)
            full = jnp.dot(both, pick_left[:, at], preferred_element_type=jnp.float32)
            even = lax.rem(lax.broadcasted_iota(jnp.int32, (1, 256), 1), 128) < 64
            left[0, :, at] = jnp.where(even, full, 0.0).astype(jnp.bfloat16)
            left[1, :, at] = jnp.where(even, 0.0, full).astype(jnp.bfloat16)

    def turn(h):
        one = jnp.full((32, 128), 1.0, jnp.float32)
        shifted = pltpu.roll(colbuf[1, 0:1, :], 96, 1)
        some = pl.ds(h * 16, 16)
        wide = rows[some, 0:24, :].reshape(HALF, 128) - jnp.where(lane < 96, colbuf[0, 0:1, :], shifted)
        u = rows[some, 24:32, :]
        rest = jnp.concatenate([u, pltpu.roll(u, 64, 2), rows[some, 32:40, :]], axis=1).reshape(HALF, 128) - shifted
        flats = [
            (jnp.transpose(wide[v * 128 : (v + 1) * 128]), jnp.transpose(rest[v * 128 : (v + 1) * 128])) for v in range(3)
        ]
        for t in range(2):
            for v in range(3):
                xyz = flats[v][0][0:96] if t == 0 else jnp.concatenate([flats[v][0][96:128], flats[v][1][0:64]], axis=0)
                sq = xyz * xyz
                m = pieces((sq[0:32] + sq[32:64]) + (sq[64:96] + 4e-10))
                p = pieces(xyz * -2.0)
                for q, (u, w) in enumerate(((one, one), (m[0], m[1]), (m[2], m[2]))):
                    for slot, rows32 in enumerate((p[q][0:32], p[q][32:64], p[q][64:96], u) + (p[q][0:32], p[q][32:64], p[q][64:96], w)):
                        right[t, q, v, slot * PITCH : slot * PITCH + 32, :] = rows32

    def distances(i, dst0, dst1):
        at = pl.ds(pl.multiple_of(i * 128, 128), 128)
        gap = jnp.zeros((16, 128), jnp.float32)
        for t in range(2):
            lhs = jnp.concatenate([left[0, t * COLS : (t + 1) * COLS, at], left[1, t * COLS : (t + 1) * COLS, at]], axis=0)
            cols = []
            for v in range(3):
                tall = []
                for s in range(2):
                    vs = [right[t, q, v, pl.ds(2 * i + s, 8, stride=PITCH), :] for q in range(3)]
                    tall += [vs[0], vs[0], vs[1], vs[1], vs[2], vs[2], gap]
                cols.append(jnp.concatenate(tall, axis=0).astype(jnp.bfloat16))
            both = jnp.dot(lhs, jnp.concatenate(cols, axis=1), preferred_element_type=jnp.float32)
            dst0[t] = both[:COLS]
            dst1[t] = both[COLS:]

    def pairs(h):
        def one(b, src):
            kept = [jnp.zeros((8, 128), jnp.float32)] * 3
            count = [jnp.zeros((8, 128), jnp.float32)] * 3
            shift = lax.rem(128 - b, 128)
            for g in range(12):
                cm = jnp.broadcast_to(pltpu.roll(colbuf[0, g * 8 : (g + 1) * 8, :], shift, 1)[:, 96:97], (8, 128))
                for v in range(3):
                    lanes = pl.ds(pl.multiple_of(h * HALF + v * 128, 128), 128)
                    w = nbuf[b, g * 8 : (g + 1) * 8, lanes].astype(jnp.float32) * cm
                    s0 = jnp.maximum(src[0, g * 8 : (g + 1) * 8, v * 128 : (v + 1) * 128], 4e-10)
                    s1 = jnp.maximum(src[1, g * 8 : (g + 1) * 8, v * 128 : (v + 1) * 128], 4e-10)
                    m = jnp.abs(s1 * lax.rsqrt(s1) - s0 * lax.rsqrt(s0))
                    score = (jnp.tanh(1.0 - m) + jnp.tanh(2.0 - m)) + (jnp.tanh(4.0 - m) + jnp.tanh(8.0 - m))
                    kept[v] = kept[v] + w * score
                    count[v] = count[v] + w
            for v in range(3):
                kept1 = jnp.sum(kept[v], axis=0, keepdims=True)
                count1 = jnp.sum(count[v], axis=0, keepdims=True)
                pr[v, pl.ds(b, 1), :] = kept1
                pr[v, pl.ds(b + 32, 1), :] = count1
                pr[v, pl.ds(b + 64, 1), :] = kept1
                pr[v, pl.ds(b + 96, 1), :] = count1

        def step(i, _):
            after = jnp.minimum(i + 1, B // 4 - 1)

            def quad(now, later):
                for j in range(4):
                    one(4 * i + j, dist.at[now + j])
                for j in range(2):
                    distances(2 * after + j, dist.at[later + 2 * j], dist.at[later + 2 * j + 1])

            @pl.when(lax.rem(i, 2) == 0)
            def _():
                quad(0, 4)

            @pl.when(lax.rem(i, 2) == 1)
            def _():
                quad(4, 0)

            return 0

        return step

    def rs_copy(h, d):
        to = h * 16 + d
        return to, pltpu.make_async_remote_copy(
            rs_send.at[to], rs_recv.at[c], rs_ssem, rs_rsem, device_id=(z, to), device_id_type=MESH
        )

    def share(h):
        low = lane < 64
        tr = [jnp.transpose(pr[g]) for g in range(3)]
        unit = lambda u: tr[u // 16][(u % 16) * 8 : (u % 16) * 8 + 8, :]
        for d in range(16):
            rs_send[h * 16 + d, 0:8, :] = jnp.where(low, unit(3 * d), unit(3 * d + 1))
            rs_send[h * 16 + d, 8:16, :] = unit(3 * d + 2)

        for d in range(16):
            to, copy = rs_copy(h, d)

            @pl.when(to != c)
            def _():
                copy.start()

            @pl.when(to == c)
            def _():
                rs_recv[c] = rs_send[c]


    left_sides()
    turn(half)
    for j in range(2):
        distances(j, dist.at[2 * j], dist.at[2 * j + 1])
    lax.fori_loop(0, SPLIT, pairs(half), 0)
    for d in range(8, 16):
        src_c = row_source(d)
        row_arrival(src_c, d)
        forward(src_c, d).start()
    lax.fori_loop(SPLIT, B // 4, pairs(half), 0)
    share(half)
    forwards_done(1)
    turn(other)
    for j in range(2):
        distances(j, dist.at[2 * j], dist.at[2 * j + 1])
    lax.fori_loop(0, B // 4, pairs(other), 0)
    share(other)

    for s in head:
        s.wait()
    feats = single[...].astype(jnp.float32)
    average = jnp.sum(feats, axis=-1, keepdims=True) * (1.0 / 384)
    centred = feats - average
    variance = jnp.sum(centred * centred, axis=-1, keepdims=True) * (1.0 / 384)
    normed = (centred * lax.rsqrt(variance + 1e-05) * gain[...].reshape(1, 384)).astype(jnp.bfloat16)
    first = jnp.maximum(jnp.dot(normed, wh[...], preferred_element_type=jnp.float32) + bh[...], 0.0).astype(jnp.bfloat16)
    second = jnp.maximum(jnp.dot(first, wm[...], preferred_element_type=jnp.float32) + bm[...], 0.0).astype(jnp.bfloat16)
    for g in range(6):
        at = lax.broadcasted_iota(jnp.int32, (1, 128), 1) + g * 128
        source = lax.bitwise_and(at, 31) * OWN + lax.shift_right_logical(at, 5)
        pick = (lax.broadcasted_iota(jnp.int32, (ROWS, 128), 0) == source).astype(jnp.float32).astype(jnp.bfloat16)
        moved = lax.dot_general(second, pick, (((0,), (0,)), ((), ())), preferred_element_type=jnp.float32)
        logits[:, g * 128 : (g + 1) * 128] = jnp.dot(wl[...], moved.astype(jnp.bfloat16), preferred_element_type=jnp.float32)
    eye = lax.broadcasted_iota(jnp.int32, (BINS, BINS), 0) == lax.broadcasted_iota(jnp.int32, (BINS, BINS), 1)
    bias = jnp.sum(jnp.where(eye, bl[...], 0.0), axis=1, keepdims=True)
    with_bias = logits[...] + bias
    logits[...] = with_bias
    top = jnp.max(with_bias, axis=0, keepdims=True)
    logz[...] = top + jnp.log(jnp.sum(jnp.exp(with_bias - top), axis=0, keepdims=True))

    everyone = lambda a, b: pltpu.make_async_remote_copy(
        rs_send.at[pl.ds(0, 31)], rs_recv.at[pl.ds(0, 31)], rs_ssem, rs_rsem, device_id=(z, partner), device_id_type=MESH
    )
    everyone(0, 0).wait_recv()
    packed = jnp.sum(rs_recv[...], axis=0)
    a0, a1 = packed[0:8], packed[8:16]
    kept = jnp.concatenate([a0, pltpu.roll(a0, 64, 1), a1], axis=0)
    count = pltpu.roll(kept, 96, 1)[:, :32] * valid
    kept = kept[:, :32] * valid
    score = (0.5 * count + 0.125 * kept) / jnp.maximum(count, 1.0)
    out[0] = score
    stats[0:24, 0:32] = score
    stats[0:24, 32:64] = score
    stats[0:24, 64:96] = score
    stats[0:24, 96:128] = score
    stats[24:48, 0:32] = valid
    stats[24:48, 32:64] = valid
    stats[24:48, 64:96] = valid
    stats[24:48, 96:128] = valid
    group = lax.shift_right_logical(lane, 5)
    centers = (lax.broadcasted_iota(jnp.int32, (BINS, 1), 0).astype(jnp.float32) + 0.5) * (1.0 / BINS)
    loss_sum = jnp.zeros((1, 128), jnp.float32)
    valid_sum = jnp.zeros((1, 128), jnp.float32)
    losses = []
    for g in range(6):
        flat = lambda base: jnp.where(
            group == 0,
            stats[base + 4 * g : base + 4 * g + 1, :],
            jnp.where(
                group == 1,
                stats[base + 4 * g + 1 : base + 4 * g + 2, :],
                jnp.where(group == 2, stats[base + 4 * g + 2 : base + 4 * g + 3, :], stats[base + 4 * g + 3 : base + 4 * g + 4, :]),
            ),
        )
        value, keep = flat(0), flat(24)
        off = value - centers
        near = jnp.exp(off * off * (-(BINS * BINS * 0.5)))
        block = logits[:, g * 128 : (g + 1) * 128]
        mean = jnp.sum(near * block, axis=0, keepdims=True) / jnp.sum(near, axis=0, keepdims=True)
        loss = keep * (logz[:, g * 128 : (g + 1) * 128] - mean)
        losses.append(loss)
        loss_sum = loss_sum + loss
        valid_sum = valid_sum + keep
    both = jnp.where(lane < 64, loss_sum + pltpu.roll(loss_sum, 64, 1), valid_sum + pltpu.roll(valid_sum, 64, 1))
    ar_send[...] = both
    me = z * 32 + c
    ar_buf[pl.ds(me, 1)] = both.reshape(1, 1, 128)
    for i in range(128):

        @pl.when(me != i)
        def _():
            pltpu.make_async_remote_copy(
                ar_send, ar_buf.at[me], ar_ssem, ar_rsem, device_id=(i // 32, i % 32), device_id_type=MESH
            ).start()

    for g in range(6):
        for t in range(4):
            part = pltpu.roll(losses[g], (128 - 32 * t) % 128, 1) if t else losses[g]
            out[1, 4 * g + t : 4 * g + t + 1, :] = part[:, :32]

    for d in range(1, 4):
        z_copy(d).wait_send()
    for d in range(4):
        to, copy = col_send(blk, d)

        @pl.when(to != c)
        def _():
            copy.wait_send()

    for d in range(1, 16):
        row_copy(d).wait_send()
    for sem in range(2):
        pltpu.make_async_remote_copy(
            rows.at[pl.ds(0, 8)], rows.at[pl.ds(0, 8)], f_ssem.at[sem], f_rsem.at[sem],
            device_id=(z, partner), device_id_type=MESH,
        ).wait_send()
    everyone(0, 0).wait_send()
    last = pltpu.make_async_remote_copy(
        ar_buf.at[pl.ds(0, 127)], ar_buf.at[pl.ds(0, 127)], ar_ssem, ar_rsem, device_id=(z, partner), device_id_type=MESH
    )
    last.wait_recv()
    everything = jnp.sum(ar_buf[...], axis=0)
    loss_total = jnp.sum(jnp.where(lane < 64, everything, 0.0), axis=1, keepdims=True)
    valid_total = jnp.sum(jnp.where(lane < 64, 0.0, everything), axis=1, keepdims=True)
    out[2] = jnp.broadcast_to(loss_total / valid_total, (OWN, B))
    last.wait_send()


def finish(out, score, loss, total):
    score[...] = out[0]
    loss[...] = out[1]
    total[...] = out[2, 0:1, 0:1]


def local(neighbor, true_coords, pred_coords, residue_mask, single, ln_gain, w_hidden, b_hidden, w_mid, b_mid, w_logits, b_logits):
    f32, bf16 = jnp.float32, jnp.bfloat16
    anywhere = pl.BlockSpec(memory_space=pl.ANY)
    in_vmem = pl.BlockSpec(memory_space=pltpu.VMEM)
    dma = pltpu.SemaphoreType.DMA
    out = pl.pallas_call(
        kernel,
        out_shape=jax.ShapeDtypeStruct((3, OWN, B), f32),
        in_specs=[anywhere] * 12,
        out_specs=in_vmem,
        scratch_shapes=[
            pltpu.VMEM((B, COLS, ROWS), jnp.int32),
            pltpu.VMEM((3, OWN, B), f32),
            pltpu.VMEM((3, OWN, B), f32),
            pltpu.VMEM((OWN, B), jnp.int32),
            pltpu.VMEM((ROWS, 384), bf16),
            pltpu.VMEM((384,), f32),
            pltpu.VMEM((384, 128), bf16),
            pltpu.VMEM((1, 128), f32),
            pltpu.VMEM((128, 128), bf16),
            pltpu.VMEM((1, 128), f32),
            pltpu.VMEM((BINS, 128), bf16),
            pltpu.VMEM((1, BINS), f32),
            pltpu.VMEM((2, OWN, 128), f32),
            pltpu.VMEM((40, 128), f32),
            pltpu.VMEM((32, 40, 128), f32),
            pltpu.VMEM((4, 2, OWN, 128), f32),
            pltpu.VMEM((2, COLS, 128), f32),
            pltpu.VMEM((512, 2048), bf16),
            pltpu.VMEM((2, 2 * COLS, 2048), bf16),
            pltpu.VMEM((2, 3, 3, 8 * PITCH, 128), f32),
            pltpu.VMEM((8, 2, COLS, HALF), f32),
            pltpu.VMEM((BINS, ROWS), f32),
            pltpu.VMEM((48, 128), f32),
            pltpu.VMEM((1, ROWS), f32),
            pltpu.VMEM((3, 128, 128), f32),
            pltpu.VMEM((32, 16, 128), f32),
            pltpu.VMEM((32, 16, 128), f32),
            pltpu.VMEM((1, 128), f32),
            pltpu.VMEM((128, 1, 128), f32),
            dma((3,)), dma((8,)), dma((8,)), dma((4,)), dma((4,)), dma((4,)), dma((4,)), dma((16,)), dma((32,)), dma((2,)), dma((2,)),
            dma, dma, dma, dma, pltpu.SemaphoreType.REGULAR,
        ],
        compiler_params=pltpu.CompilerParams(collective_id=0, has_side_effects=True, vmem_limit_bytes=67043328),
    )(
        neighbor,
        jnp.transpose(true_coords, (1, 2, 0)),
        jnp.transpose(pred_coords, (1, 2, 0)),
        residue_mask.T,
        single.reshape(ROWS, 384),
        ln_gain,
        w_hidden,
        b_hidden.reshape(1, 128),
        w_mid,
        b_mid.reshape(1, 128),
        w_logits.T,
        b_logits.reshape(1, BINS),
    )
    score, loss, total = pl.pallas_call(
        finish,
        out_shape=(jax.ShapeDtypeStruct((OWN, B), f32), jax.ShapeDtypeStruct((OWN, B), f32), jax.ShapeDtypeStruct((1, 1), f32)),
        in_specs=[in_vmem],
        out_specs=(in_vmem, in_vmem, in_vmem),
    )(out)
    return score.T, loss.T, total.reshape(())


def solution(mesh):
    placed = (
        P(None, "col", "row"),
        P(None, None, ("row", "col")),
        P(None, None, ("row", "col")),
        P(None, ("row", "col")),
        P(None, ("row", "col"), None),
    ) + (P(),) * 7
    return jax.shard_map(
        local,
        mesh=mesh,
        in_specs=placed,
        out_specs=(P(None, ("row", "col")), P(None, ("row", "col")), P()),
        check_vma=False,
    )
```
